32 devices in a mesh: rep: 2 (over x), dp: 16 (over y, z, core).
Axes of the slice: x: 2, y: 2, z: 4, core: 2. Of those that a mesh axis runs over, the one named last changes fastest.
Arguments:
- a: bfloat16 [32, 4, 4096, 1280], P(('rep', 'dp')), parts along dimension 0
- g: bfloat16 [32, 4, 4096, 3072], P(('rep', 'dp')), parts along dimension 0
Outputs:
- output: bfloat16 [8, 1280, 3072], P('rep'), parts along dimension 0
There are 2 independent parts. The reference program is written for one: setup_inputs(seed, part) draws one part's arguments, and reference() takes and returns one part's arrays. A program takes and returns all parts, laid end to end along the dimension named above; each array names one.
All inputs are finite; a program needn't handle non-finite values.
Results may differ from the reference program's by a relative error of at most 0.012.
Values are sent between devices in bfloat16 or wider.
A program may use at most 2 GiB of HBM per device.

```python
import jax
import jax.numpy as jnp
from jax import lax

DEVICES = 16
MATRICES = 4
TOKENS = 4096
D = 1280
FF = 3072


def setup_inputs(seed: int = 0, part: int = 0) -> dict:
    ka, kg, ks = (jax.random.fold_in(k, part) for k in jax.random.split(jax.random.key(seed), 3))
    size = 2.0 ** jax.random.uniform(ks, (DEVICES, MATRICES, 1, 1), jnp.float32, -1.0, 1.0)
    a = jax.random.normal(ka, (DEVICES, MATRICES, TOKENS, D), jnp.float32)
    g = size * jax.random.normal(kg, (DEVICES, MATRICES, TOKENS, FF), jnp.float32) * (DEVICES * TOKENS) ** -0.5
    return {"a": a.astype(jnp.bfloat16), "g": g.astype(jnp.bfloat16)}


def reference(a, g):
    def take(so_far, one):
        return so_far + jnp.einsum("ntd,ntf->ndf", *one, preferred_element_type=jnp.float32), None

    return lax.scan(take, jnp.zeros((MATRICES, D, FF), jnp.float32), (a, g))[0].astype(jnp.bfloat16)
```

```python
import jax
import jax.numpy as jnp
from jax import lax
from jax.experimental import pallas as pl
from jax.experimental.pallas import tpu as pltpu
from jax.sharding import PartitionSpec as P

MESH = pl.DeviceIdType.MESH
BF16, F32 = jnp.bfloat16, jnp.float32
W = 256
FIN = 12
DN = (((0,), (0,)), ((), ()))


def kernel(mats, per_mat, a_hbm, g_hbm, out_hbm, a_v, g_v, part, d_s, d_r, y_s, y_r, y_own, za_s, za_r, z_own, zb_s, zb_r,
           zc_s, zc_r, zd_s, zd_r, yz_s, yz_r, fin, a_sem, g_sem, w_sem, sem4s, sem4r, sem8s, sem8r, sem12s, sem12r):
    units = mats * per_mat
    rows = a_v.shape[2]
    half = rows // 2
    q = half // 4
    dp = lax.axis_index("dp")
    y, z, c = dp // 8, (dp // 2) % 4, dp % 2
    mid = jnp.logical_or(z == 1, z == 2)
    end = jnp.logical_not(mid)
    root = jnp.where(z == 2, 1, 0)
    partner = dp + 1 - 2 * c
    yn = dp + 8 - 16 * y
    adj = dp + 2 - 4 * (z % 2)
    om = jnp.where(mid, dp + 6 - 4 * z, dp)

    def at(n):
        return pl.ds(pl.multiple_of(n, 16), q)

    mine = pl.ds(pl.multiple_of(c * half, 16), half)
    theirs = pl.ds(pl.multiple_of((1 - c) * half, 16), half)
    yrow = at(c * half + y * q)
    yrow_other = at(c * half + (1 - y) * q)
    zrow = at(c * half + 2 * q + root * q)
    zrow_other = at(c * half + 2 * q + (1 - root) * q)
    adj_root = jnp.where(z >= 2, 1, 0)
    erow_near = at(c * half + 2 * q + adj_root * q)
    erow_far = at(c * half + 2 * q + (1 - adj_root) * q)

    def rdma(src, dst, ss, rs, to):
        return pltpu.make_async_remote_copy(src_ref=src, dst_ref=dst, send_sem=ss, recv_sem=rs, device_id={"dp": to}, device_id_type=MESH)

    def s4(kind, u):
        return sem4s.at[kind, u % 4], sem4r.at[kind, u % 4]

    def s8(kind, u):
        return sem8s.at[kind, u % 8], sem8r.at[kind, u % 8]

    def s12(kind, u):
        return sem12s.at[kind, u % FIN], sem12r.at[kind, u % FIN]

    d_copy = lambda u: rdma(d_s.at[u % 4], d_r.at[u % 4], *s4(0, u), partner)
    y_copy = lambda u: rdma(y_s.at[u % 4], y_r.at[u % 4], *s4(1, u), yn)
    zc_copy = lambda u: rdma(zc_s.at[u % 4], zc_r.at[u % 4], *s4(2, u), om)
    zd_copy = lambda u: rdma(zd_s.at[u % 4], zd_r.at[u % 4], *s4(3, u), om)
    yz_copy = lambda u: rdma(yz_s.at[u % 4], yz_r.at[u % 4], *s4(4, u), yn)
    za_copy = lambda u: rdma(za_s.at[u % 4], za_r.at[u % 8], *s8(0, u), adj)
    zb_copy = lambda u: rdma(zb_s.at[u % 4], zb_r.at[u % 8], *s8(1, u), adj)

    def fin_copy(kind, r, to):
        return lambda u: rdma(fin.at[u % FIN, r], fin.at[u % FIN, r], *s12(kind, u), to)

    z3_copy = fin_copy(0, yrow, adj)
    near_copy = fin_copy(1, zrow, adj)
    near_in = fin_copy(1, erow_near, adj)
    cross_copy = fin_copy(2, zrow, om)
    cross_in = fin_copy(2, zrow_other, om)
    far_copy = fin_copy(3, zrow_other, adj)
    far_in = fin_copy(3, erow_far, adj)
    ag_copy = fin_copy(4, yrow, yn)
    ag_in = fin_copy(4, yrow_other, yn)
    df_copy = fin_copy(5, mine, partner)
    df_in = fin_copy(5, theirs, partner)

    def out_at(u):
        return out_hbm.at[u // per_mat, :, pl.ds(pl.multiple_of((u % per_mat) * W, W), W)]

    w_copy = lambda u: pltpu.make_async_copy(fin.at[u % FIN], out_at(u), w_sem.at[u % FIN])
    a_copy = lambda n: pltpu.make_async_copy(a_hbm.at[0, n], a_v.at[n % 2], a_sem.at[n % 2])

    def g_copy(u):
        src = g_hbm.at[0, u // per_mat, :, pl.ds(pl.multiple_of((u % per_mat) * W, W), W)]
        return pltpu.make_async_copy(src, g_v.at[u % 3], g_sem.at[u % 3])

    a_copy(0).start()
    g_copy(0).start()
    g_copy(1).start()

    def step(t, _):
        def stage(off):
            u = t - off
            return u, jnp.logical_and(u >= 0, u < units)

        u8, on8 = stage(14)

        @pl.when(on8)
        def _():
            w_copy(u8).wait()

        u7, on7 = stage(12)

        @pl.when(on7)
        def _():
            df_copy(u7).wait_send()
            df_in(u7).wait_recv()
            w_copy(u7).start()

        u6, on6 = stage(11)

        @pl.when(on6)
        def _():
            ag_copy(u6).wait_send()
            ag_in(u6).wait_recv()

            @pl.when(mid)
            def _():
                far_copy(u6).wait_send()

            @pl.when(end)
            def _():
                far_in(u6).wait_recv()

            df_copy(u6).start()

        u5, on5 = stage(9)

        @pl.when(on5)
        def _():
            @pl.when(mid)
            def _():
                cross_in(u5).wait_recv()
                far_copy(u5).start()
                z3_copy(u5).wait_send()
                ag_copy(u5).start()
                near_copy(u5).wait_send()
                cross_copy(u5).wait_send()

            @pl.when(end)
            def _():
                z3_copy(u5).wait_recv()
                ag_copy(u5).start()
                near_in(u5).wait_recv()

        u4, on4 = stage(7)

        @pl.when(jnp.logical_and(on4, mid))
        def _():
            k = u4 % 4
            zd_copy(u4).wait()
            fin[u4 % FIN, yrow, :] = (zd_s[k].astype(F32) + zd_r[k].astype(F32)).astype(BF16)
            z3_copy(u4).start()
            yz_copy(u4).wait()
            fin[u4 % FIN, zrow, :] = (yz_s[k].astype(F32) + yz_r[k].astype(F32)).astype(BF16)
            near_copy(u4).start()
            cross_copy(u4).start()

        u3, on3 = stage(5)

        @pl.when(jnp.logical_and(on3, mid))
        def _():
            k = u3 % 4
            zb_copy(u3).wait_recv()
            zd_s[k] = (y_own[k] + zb_r[u3 % 8].astype(F32)).astype(BF16)
            zd_copy(u3).start()
            zc_copy(u3).wait()
            yz_s[k] = (z_own[k, at(root * q), :] + zc_r[k].astype(F32)).astype(BF16)
            yz_copy(u3).start()

        @pl.when(jnp.logical_and(on3, end))
        def _():
            zb_copy(u3).wait_send()

        u2, on2 = stage(3)

        @pl.when(on2)
        def _():
            k = u2 % 4
            y_copy(u2).wait()

            @pl.when(end)
            def _():
                zb_s[k] = (y_own[k] + y_r[k].astype(F32)).astype(BF16)
                zb_copy(u2).start()
                za_copy(u2).wait_send()

            @pl.when(mid)
            def _():
                y_own[k] = y_own[k] + y_r[k].astype(F32)
                za_copy(u2).wait_recv()
                other = at((1 - root) * q)
                own = at(root * q)
                zc_s[k] = (z_own[k, other, :] + za_r[u2 % 8, other, :].astype(F32)).astype(BF16)
                zc_copy(u2).start()
                z_own[k, own, :] = z_own[k, own, :] + za_r[u2 % 8, own, :].astype(F32)

        @pl.when(t < units)
        def _():
            n = t // per_mat

            @pl.when(t % per_mat == 0)
            def _():
                a_copy(n).wait()

                @pl.when(n + 1 < mats)
                def _():
                    a_copy(n + 1).start()

            g_copy(t).wait()

            @pl.when(t + 2 < units)
            def _():
                g_copy(t + 2).start()

            def block(j, _):
                cols = pl.ds(pl.multiple_of(j * half, 128), half)
                part[t % 2, pl.ds(pl.multiple_of(j * half, 16), half), :] = lax.dot_general(
                    a_v[n % 2, :, cols], g_v[t % 3], DN, preferred_element_type=F32)
                return 0

            lax.fori_loop(0, 2, block, 0)
            d_s[t % 4] = part[t % 2, theirs, :].astype(BF16)
            d_copy(t).start()

        u1, on1 = stage(1)

        @pl.when(on1)
        def _():
            k = u1 % 4
            p = u1 % 2
            d_copy(u1).wait()
            there = (1 - y) * q
            here = y * q
            y_s[k] = (part[p, at(c * half + there), :] + d_r[k, at(there), :].astype(F32)).astype(BF16)
            y_copy(u1).start()
            zpart = pl.ds(pl.multiple_of(c * half + 2 * q, 16), 2 * q)

            @pl.when(end)
            def _():
                za_s[k] = (part[p, zpart, :] + d_r[k, 2 * q:, :].astype(F32)).astype(BF16)
                za_copy(u1).start()

            @pl.when(mid)
            def _():
                z_own[k] = part[p, zpart, :] + d_r[k, 2 * q:, :].astype(F32)

            y_own[k] = part[p, at(c * half + here), :] + d_r[k, at(here), :].astype(F32)

        return 0

    lax.fori_loop(0, units + 15, step, 0)


def solution(mesh):
    def local(a, g):
        _, mats, tokens, rows = a.shape
        cols = g.shape[3]
        half = rows // 2
        q = half // 4

        def buf(slots, n, dtype=BF16):
            return pltpu.VMEM((slots, n, W), dtype)

        def body(*refs):
            kernel(mats, cols // W, *refs)

        any_spec = pl.BlockSpec(memory_space=pl.ANY)
        dma = pltpu.SemaphoreType.DMA
        return pl.pallas_call(
            body,
            out_shape=jax.ShapeDtypeStruct((mats, rows, cols), BF16),
            in_specs=[any_spec, any_spec],
            out_specs=any_spec,
            scratch_shapes=[
                pltpu.VMEM((2, tokens, rows), BF16),
                pltpu.VMEM((3, tokens, W), BF16),
                buf(2, rows, F32),
                buf(4, half), buf(4, half),
                buf(4, q), buf(4, q), buf(4, q, F32),
                buf(4, 2 * q), buf(8, 2 * q), buf(4, 2 * q, F32),
                buf(4, q), buf(8, q),
                buf(4, q), buf(4, q),
                buf(4, q), buf(4, q),
                buf(4, q), buf(4, q),
                buf(FIN, rows),
                dma((2,)), dma((3,)), dma((FIN,)),
                dma((5, 4)), dma((5, 4)),
                dma((2, 8)), dma((2, 8)),
                dma((6, FIN)), dma((6, FIN)),
            ],
            compiler_params=pltpu.CompilerParams(has_side_effects=True, vmem_limit_bytes=60 * 2**20),
            cost_estimate=pl.CostEstimate(flops=2 * mats * tokens * rows * cols, bytes_accessed=2 * mats * tokens * (rows + cols), transcendentals=0),
        )(a, g)

    spec = P(("rep", "dp"))
    return jax.shard_map(local, mesh=mesh, in_specs=(spec, spec), out_specs=P("rep"), check_vma=False)
```

```python
import jax
import jax.numpy as jnp
from jax import lax
from jax.experimental import pallas as pl
from jax.experimental.pallas import tpu as pltpu
from jax.sharding import PartitionSpec as P

MESH = pl.DeviceIdType.MESH
BF16, F32 = jnp.bfloat16, jnp.float32
W = 256
PARTS = 2
SLOTS = 8
LAG = 2
DN = (((0,), (0,)), ((), ()))


def kernel(mats, q, zq, a_hbm, g_hbm, out, a_v, g_v, part, d_s, d_r, y_s, y_r, y_own, za_s, za_r, z_own, zb_s, zb_r,
           zm_s, zm_r, zd_s, zd_r, ze_s, ze_r, yz_s, yz_r, a_sem, g_sem, send_sem, recv_sem):
    rows = a_v.shape[2]
    half = rows // 2
    per_row = out.shape[2] // W
    units = mats * PARTS * per_row
    dp = lax.axis_index("dp")
    y, z, c = dp // 8, (dp // 2) % 4, dp % 2
    mid = jnp.logical_or(z == 1, z == 2)
    end = jnp.logical_not(mid)
    side = z // 2
    partner = dp + 1 - 2 * c
    yn = dp + 8 - 16 * y
    adj = dp + 2 - 4 * (z % 2)
    om = jnp.where(mid, dp + 6 - 4 * z, dp)
    r_adj = z + 1 - 2 * (z % 2)
    r_om = 3 - z
    r_far = r_om + 1 - 2 * (r_om % 2)

    def span(start, n):
        return pl.ds(pl.multiple_of(start, 16), n)

    def rdma(kind, src, dst, u, to):
        return pltpu.make_async_remote_copy(
            src_ref=src, dst_ref=dst, send_sem=send_sem.at[kind, u % SLOTS], recv_sem=recv_sem.at[kind, u % SLOTS],
            device_id={"dp": to}, device_id_type=MESH)

    def place(u):
        n = u // (PARTS * per_row)
        return n, (u // per_row) % PARTS, pl.ds(pl.multiple_of((u % per_row) * W, W), W)

    def out_at(u, core, start, n):
        m, p, cols = place(u)
        return out.at[m, span(p * rows + core * half + start, n), cols]

    def final_copy(kind, core, start, n, to):
        def make(u):
            ref = out_at(u, core, start, n)
            return rdma(kind, ref, ref, u, to)

        return make

    def piece(r):
        return 2 * q + r * zq

    d_copy = lambda u: rdma(0, d_s.at[u % 4], d_r.at[u % SLOTS], u, partner)
    y_copy = lambda u: rdma(1, y_s.at[u % 4], y_r.at[u % SLOTS], u, yn)
    near_rows = span((1 - side) * zq, 3 * zq)
    za_copy = lambda u: rdma(2, za_s.at[u % 4], za_r.at[u % SLOTS, near_rows], u, adj)
    zb_copy = lambda u: rdma(3, zb_s.at[u % 4], zb_r.at[u % SLOTS], u, adj)
    zm_copy = lambda u: rdma(4, zm_s.at[u % 4], zm_r.at[u % SLOTS], u, om)
    zd_copy = lambda u: rdma(5, zd_s.at[u % 4], zd_r.at[u % SLOTS], u, om)
    ze_copy = lambda u: rdma(6, ze_s.at[u % 4], ze_r.at[u % SLOTS], u, adj)
    yz_copy = lambda u: rdma(7, yz_s.at[u % 4], yz_r.at[u % SLOTS], u, yn)
    z3_copy = final_copy(8, c, y * q, q, adj)
    ag_copy = final_copy(9, c, y * q, q, yn)
    ag_in = final_copy(9, c, (1 - y) * q, q, yn)
    near_copy = final_copy(10, c, piece(z), zq, adj)
    near_in = final_copy(10, c, piece(r_adj), zq, adj)
    cross_copy = final_copy(11, c, piece(z), zq, om)
    cross_in = final_copy(11, c, piece(r_om), zq, om)
    up_copy = final_copy(12, c, piece(z), zq, adj)
    up_in = final_copy(12, c, piece(r_adj), zq, adj)
    far1_copy = final_copy(13, c, piece(r_om), zq, adj)
    far1_in = final_copy(13, c, piece(r_far), zq, adj)
    over_copy = final_copy(14, c, piece(r_adj), zq, om)
    over_in = final_copy(14, c, piece(r_far), zq, om)
    far2_copy = final_copy(15, c, piece(r_far), zq, adj)
    far2_in = final_copy(15, c, piece(r_om), zq, adj)
    df_copy = final_copy(16, c, 0, half, partner)
    df_in = final_copy(16, 1 - c, 0, half, partner)

    def a_copy(i):
        src = a_hbm.at[0, i // PARTS, :, pl.ds(pl.multiple_of((i % PARTS) * rows, 128), rows)]
        return pltpu.make_async_copy(src, a_v.at[i % 2], a_sem.at[i % 2])

    def g_copy(u):
        m, _, cols = place(u)
        return pltpu.make_async_copy(g_hbm.at[0, m, :, cols], g_v.at[u % 3], g_sem.at[u % 3])

    def store(u, start, n, value):
        m, p, cols = place(u)
        out[m, span(p * rows + c * half + start, n), cols] = value.astype(BF16)

    a_copy(0).start()
    g_copy(0).start()
    g_copy(1).start()

    def step(t, _):
        def stage(off, who=None):
            u = t - off
            on = jnp.logical_and(u >= 0, u < units)
            return u, pl.when(on if who is None else jnp.logical_and(on, who))

        u, when = stage(2 + 7 * LAG)

        @when
        def _(u=u):
            df_copy(u).wait_send()
            df_in(u).wait_recv()

        u, when = stage(1 + 7 * LAG, mid)

        @when
        def _(u=u):
            far2_copy(u).wait_send()
            df_copy(u).start()

        u, when = stage(1 + 7 * LAG, end)

        @when
        def _(u=u):
            far2_in(u).wait_recv()
            df_copy(u).start()

        u, when = stage(1 + 6 * LAG, mid)

        @when
        def _(u=u):
            over_in(u).wait_recv()
            far2_copy(u).start()
            over_copy(u).wait_send()

        u, when = stage(1 + 5 * LAG)

        @when
        def _(u=u):
            @pl.when(mid)
            def _():
                up_in(u).wait_recv()
                over_copy(u).start()
                far1_copy(u).wait_send()

            @pl.when(end)
            def _():
                far1_in(u).wait_recv()
                up_copy(u).wait_send()

            ag_copy(u).wait_send()
            ag_in(u).wait_recv()

        u, when = stage(1 + 4 * LAG, mid)

        @when
        def _(u=u):
            z3_copy(u).wait_send()
            ag_copy(u).start()
            cross_in(u).wait_recv()
            far1_copy(u).start()
            near_copy(u).wait_send()
            cross_copy(u).wait_send()

        u, when = stage(1 + 4 * LAG, end)

        @when
        def _(u=u):
            z3_copy(u).wait_recv()
            ag_copy(u).start()
            yz_copy(u).wait()
            store(u, piece(z), zq, yz_s[u % 4].astype(F32) + yz_r[u % SLOTS].astype(F32))
            up_copy(u).start()
            near_in(u).wait_recv()

        u, when = stage(1 + 3 * LAG, mid)

        @when
        def _(u=u):
            zd_copy(u).wait()
            store(u, y * q, q, zd_s[u % 4].astype(F32) + zd_r[u % SLOTS].astype(F32))
            z3_copy(u).start()
            yz_copy(u).wait()
            store(u, piece(z), zq, yz_s[u % 4].astype(F32) + yz_r[u % SLOTS].astype(F32))
            near_copy(u).start()
            cross_copy(u).start()
            ze_copy(u).wait_send()

        u, when = stage(1 + 3 * LAG, end)

        @when
        def _(u=u):
            ze_copy(u).wait_recv()
            k = u % SLOTS
            yz_s[u % 4] = (z_own[k, span(z * zq, zq)] + ze_r[k].astype(F32)).astype(BF16)
            yz_copy(u).start()

        u, when = stage(1 + 2 * LAG, mid)

        @when
        def _(u=u):
            k = u % SLOTS
            zb_copy(u).wait_recv()
            zd_s[u % 4] = (y_own[k] + zb_r[k].astype(F32)).astype(BF16)
            zd_copy(u).start()
            zm_copy(u).wait()
            ze_s[u % 4] = (z_own[k, span(r_adj * zq, zq)] + zm_r[k, span((r_adj % 2) * zq, zq)].astype(F32)).astype(BF16)
            ze_copy(u).start()
            mine = span(z * zq, zq)
            yz_s[u % 4] = (z_own[k, mine] + za_r[k, mine].astype(F32) + zm_r[k, span((z % 2) * zq, zq)].astype(F32)).astype(BF16)
            yz_copy(u).start()

        u, when = stage(1 + 2 * LAG, end)

        @when
        def _(u=u):
            zb_copy(u).wait_send()

        u, when = stage(1 + LAG)

        @when
        def _(u=u):
            k = u % SLOTS
            y_copy(u).wait()

            @pl.when(end)
            def _():
                zb_s[u % 4] = (y_own[k] + y_r[k].astype(F32)).astype(BF16)
                zb_copy(u).start()
                za_copy(u).wait_send()

            @pl.when(mid)
            def _():
                za_copy(u).wait_recv()
                other = span((1 - side) * 2 * zq, 2 * zq)
                zm_s[u % 4] = (z_own[k, other] + za_r[k, other].astype(F32)).astype(BF16)
                zm_copy(u).start()
                y_own[k] = y_own[k] + y_r[k].astype(F32)

        @pl.when(t < units)
        def _():
            i = t // per_row

            @pl.when(t % per_row == 0)
            def _():
                a_copy(i).wait()

                @pl.when(i + 1 < mats * PARTS)
                def _():
                    a_copy(i + 1).start()

            g_copy(t).wait()

            @pl.when(t + 2 < units)
            def _():
                g_copy(t + 2).start()

            part[t % 2] = lax.dot_general(a_v[i % 2], g_v[t % 3], DN, preferred_element_type=F32)
            d_s[t % 4] = part[t % 2, span((1 - c) * half, half), :].astype(BF16)
            d_copy(t).start()

        u, when = stage(1)

        @when
        def _(u=u):
            k = u % SLOTS
            p = u % 2
            d_copy(u).wait()
            there = (1 - y) * q
            here = y * q
            y_s[u % 4] = (part[p, span(c * half + there, q)] + d_r[k, span(there, q)].astype(F32)).astype(BF16)
            y_copy(u).start()

            @pl.when(end)
            def _():
                start = 2 * q + (1 - side) * zq
                za_s[u % 4] = (part[p, span(c * half + start, 3 * zq)] + d_r[k, span(start, 3 * zq)].astype(F32)).astype(BF16)
                za_copy(u).start()

            y_own[k] = part[p, span(c * half + here, q)] + d_r[k, span(here, q)].astype(F32)
            z_own[k] = part[p, span(c * half + 2 * q, 4 * zq)] + d_r[k, 2 * q:].astype(F32)

        return 0

    lax.fori_loop(0, units + 3 + 7 * LAG, step, 0)


def write(x, out, sems):
    copies = [pltpu.make_async_copy(x.at[n], out.at[n], sems.at[n]) for n in range(out.shape[0])]
    for copy in copies:
        copy.start()
    for copy in copies:
        copy.wait()


def solution(mesh):
    def local(a, g):
        _, mats, tokens, depth = a.shape
        cols = g.shape[3]
        rows = depth // PARTS
        half = rows // 2
        zq = half // 10
        q = 3 * zq

        def buf(slots, n, dtype=BF16):
            return pltpu.VMEM((slots, n, W), dtype)

        def body(*refs):
            kernel(mats, q, zq, *refs)

        any_spec = pl.BlockSpec(memory_space=pl.ANY)
        dma = pltpu.SemaphoreType.DMA
        sums = pl.pallas_call(
            body,
            out_shape=pltpu.VMEM((mats, depth, cols), BF16),
            in_specs=[any_spec, any_spec],
            out_specs=pl.BlockSpec(memory_space=pltpu.VMEM),
            scratch_shapes=[
                pltpu.VMEM((2, tokens, rows), BF16),
                pltpu.VMEM((3, tokens, W), BF16),
                buf(2, rows, F32),
                buf(4, half), buf(SLOTS, half),
                buf(4, q), buf(SLOTS, q), buf(SLOTS, q, F32),
                buf(4, 3 * zq), buf(SLOTS, 4 * zq), buf(SLOTS, 4 * zq, F32),
                buf(4, q), buf(SLOTS, q),
                buf(4, 2 * zq), buf(SLOTS, 2 * zq),
                buf(4, q), buf(SLOTS, q),
                buf(4, zq), buf(SLOTS, zq),
                buf(4, zq), buf(SLOTS, zq),
                dma((2,)), dma((3,)),
                dma((17, SLOTS)), dma((17, SLOTS)),
            ],
            compiler_params=pltpu.CompilerParams(has_side_effects=True, vmem_limit_bytes=31 * 2**20),
            cost_estimate=pl.CostEstimate(flops=2 * mats * tokens * depth * cols, bytes_accessed=2 * mats * tokens * (depth + cols), transcendentals=0),
        )(a, g)
        return pl.pallas_call(
            write,
            out_shape=jax.ShapeDtypeStruct((mats, depth, cols), BF16),
            in_specs=[any_spec],
            out_specs=any_spec,
            scratch_shapes=[dma((mats,))],
            compiler_params=pltpu.CompilerParams(vmem_limit_bytes=2**20),
        )(sums)

    spec = P(("rep", "dp"))
    return jax.shard_map(local, mesh=mesh, in_specs=(spec, spec), out_specs=P("rep"), check_vma=False)
```

```python
import jax
import jax.numpy as jnp
from jax import lax
from jax.experimental import pallas as pl
from jax.experimental.pallas import tpu as pltpu
from jax.sharding import PartitionSpec as P

MESH = pl.DeviceIdType.MESH
BF16, F32 = jnp.bfloat16, jnp.float32
W = 256
PARTS = 2
SLOTS = 8
SEMS = 16
LATE = 3
CHUNKS = 4
LAG = 2
WRITES = 4
DN = (((0,), (0,)), ((), ()))


def kernel(mats, q, zq, a_hbm, g_hbm, out, a_v, g_v, part, d_s, d_r, y_s, y_r, y_own, za_s, za_r, z_own, zb_s, zb_r,
           zm_s, zm_r, zd_s, zd_r, ze_s, ze_r, yz_s, yz_r, a_sem, g_sem, first_sem, send_sem, recv_sem):
    rows = a_v.shape[2]
    half = rows // 2
    per_row = out.shape[2] // W
    units = mats * PARTS * per_row
    dp = lax.axis_index("dp")
    y, z, c = dp // 8, (dp // 2) % 4, dp % 2
    mid = jnp.logical_or(z == 1, z == 2)
    end = jnp.logical_not(mid)
    side = z // 2
    partner = dp + 1 - 2 * c
    yn = dp + 8 - 16 * y
    adj = dp + 2 - 4 * (z % 2)
    om = jnp.where(mid, dp + 6 - 4 * z, dp)
    r_adj = z + 1 - 2 * (z % 2)
    r_om = 3 - z
    r_far = r_om + 1 - 2 * (r_om % 2)

    far_mid = dp + 2 * (r_far - z)
    far_end = dp + 2 * (r_om - z)

    def span(start, n):
        return pl.ds(pl.multiple_of(start, 16), n)

    def rdma(kind, src, dst, u, to):
        return pltpu.make_async_remote_copy(
            src_ref=src, dst_ref=dst, send_sem=send_sem.at[kind, u % SEMS], recv_sem=recv_sem.at[kind, u % SEMS],
            device_id={"dp": to}, device_id_type=MESH)

    def place(u):
        n = u // (PARTS * per_row)
        return n, (u // per_row) % PARTS, pl.ds(pl.multiple_of((u % per_row) * W, W), W)

    def out_at(u, core, start, n):
        m, p, cols = place(u)
        return out.at[m, span(p * rows + core * half + start, n), cols]

    def final_copy(kind, core, start, n, to):
        def make(u):
            ref = out_at(u, core, start, n)
            return rdma(kind, ref, ref, u, to)

        return make

    def piece(r):
        return 2 * q + r * zq

    d_copy = lambda u: rdma(0, d_s.at[u % 4], d_r.at[u % SLOTS], u, partner)
    y_copy = lambda u: rdma(1, y_s.at[u % 4], y_r.at[u % SLOTS], u, yn)
    near_rows = span((1 - side) * zq, 3 * zq)
    za_copy = lambda u: rdma(2, za_s.at[u % 4], za_r.at[u % SLOTS, near_rows], u, adj)
    zb_copy = lambda u: rdma(3, zb_s.at[u % 4], zb_r.at[u % SLOTS], u, adj)
    zm_copy = lambda u: rdma(4, zm_s.at[u % 4], zm_r.at[u % SLOTS], u, om)
    zd_copy = lambda u: rdma(5, zd_s.at[u % 4], zd_r.at[u % SLOTS], u, om)
    ze_copy = lambda u: rdma(6, ze_s.at[u % 4], ze_r.at[u % SLOTS], u, adj)
    yz_copy = lambda u: rdma(7, yz_s.at[u % 4], yz_r.at[u % SLOTS], u, yn)
    z3_copy = final_copy(8, c, y * q, q, adj)
    ag_copy = final_copy(9, c, y * q, q, yn)
    ag_in = final_copy(9, c, (1 - y) * q, q, yn)
    near_copy = final_copy(10, c, piece(z), zq, adj)
    near_in = final_copy(10, c, piece(r_adj), zq, adj)
    cross_copy = final_copy(11, c, piece(z), zq, om)
    cross_in = final_copy(11, c, piece(r_om), zq, om)
    up_copy = final_copy(12, c, piece(z), zq, adj)
    up_in = final_copy(12, c, piece(r_adj), zq, adj)
    far1_copy = final_copy(13, c, piece(r_om), zq, adj)
    far1_in = final_copy(13, c, piece(r_far), zq, adj)
    over_copy = final_copy(14, c, piece(r_adj), zq, om)
    over_in = final_copy(14, c, piece(r_far), zq, om)
    far2_copy = final_copy(15, c, piece(r_far), zq, adj)
    far2_in = final_copy(15, c, piece(r_om), zq, adj)
    over_late = final_copy(14, c, piece(z), zq, far_mid)
    far2_late = final_copy(15, c, piece(z), zq, far_end)
    df_copy = final_copy(16, c, 0, half, partner)
    df_in = final_copy(16, 1 - c, 0, half, partner)

    def a_copy(i):
        src = a_hbm.at[0, i // PARTS, :, pl.ds(pl.multiple_of((i % PARTS) * rows, 128), rows)]
        return pltpu.make_async_copy(src, a_v.at[i % 2], a_sem.at[i % 2])

    def g_copy(u):
        m, _, cols = place(u)
        return pltpu.make_async_copy(g_hbm.at[0, m, :, cols], g_v.at[u % 3], g_sem.at[u % 3])

    def store(u, start, n, value):
        m, p, cols = place(u)
        out[m, span(p * rows + c * half + start, n), cols] = value.astype(BF16)

    tokens = a_v.shape[1] // CHUNKS

    def first_copies(i):
        some = span(i * tokens, tokens)
        return (pltpu.make_async_copy(a_hbm.at[0, 0, some, pl.ds(0, rows)], a_v.at[0, some], first_sem.at[0, i]),
                pltpu.make_async_copy(g_hbm.at[0, 0, some, pl.ds(0, W)], g_v.at[0, some], first_sem.at[1, i]))

    for i in range(CHUNKS):
        for copy in first_copies(i):
            copy.start()
    a_copy(1).start()
    g_copy(1).start()

    barrier = pltpu.get_barrier_semaphore()
    peers = [partner, yn] + [dp + 2 * ((z + i) % 4 - z) for i in range(1, 4)]
    for peer in peers:
        pl.semaphore_signal(barrier, inc=1, device_id={"dp": peer}, device_id_type=MESH)
    pl.semaphore_wait(barrier, len(peers))

    def step(t, _):
        def stage(off, who=None):
            u = t - off
            on = jnp.logical_and(u >= 0, u < units)
            return u, pl.when(on if who is None else jnp.logical_and(on, who))

        u, when = stage(2 + 7 * LAG)

        @when
        def _(u=u):
            df_copy(u).wait_send()
            df_in(u).wait_recv()

        u, when = stage(1 + 7 * LAG, mid)

        @when
        def _(u=u):
            @pl.when(u < units - LATE)
            def _():
                far2_copy(u).wait_send()

            df_copy(u).start()

        u, when = stage(1 + 7 * LAG, end)

        @when
        def _(u=u):
            far2_in(u).wait_recv()
            df_copy(u).start()

        u, when = stage(1 + 6 * LAG, mid)

        @when
        def _(u=u):
            over_in(u).wait_recv()

            @pl.when(u < units - LATE)
            def _():
                far2_copy(u).start()
                over_copy(u).wait_send()

        u, when = stage(1 + 5 * LAG)

        @when
        def _(u=u):
            @pl.when(mid)
            def _():
                up_in(u).wait_recv()

                @pl.when(u < units - LATE)
                def _():
                    over_copy(u).start()

                far1_copy(u).wait_send()

            @pl.when(end)
            def _():
                far1_in(u).wait_recv()
                up_copy(u).wait_send()

                @pl.when(u >= units - LATE)
                def _():
                    over_late(u).wait_send()
                    far2_late(u).wait_send()

            ag_copy(u).wait_send()
            ag_in(u).wait_recv()

        u, when = stage(1 + 4 * LAG, mid)

        @when
        def _(u=u):
            z3_copy(u).wait_send()
            ag_copy(u).start()
            cross_in(u).wait_recv()
            far1_copy(u).start()
            near_copy(u).wait_send()
            cross_copy(u).wait_send()

        u, when = stage(1 + 4 * LAG, end)

        @when
        def _(u=u):
            z3_copy(u).wait_recv()
            ag_copy(u).start()
            yz_copy(u).wait()
            store(u, piece(z), zq, yz_s[u % 4].astype(F32) + yz_r[u % SLOTS].astype(F32))
            up_copy(u).start()

            @pl.when(u >= units - LATE)
            def _():
                over_late(u).start()
                far2_late(u).start()

            near_in(u).wait_recv()

        u, when = stage(1 + 3 * LAG, mid)

        @when
        def _(u=u):
            zd_copy(u).wait()
            store(u, y * q, q, zd_s[u % 4].astype(F32) + zd_r[u % SLOTS].astype(F32))
            z3_copy(u).start()
            yz_copy(u).wait()
            store(u, piece(z), zq, yz_s[u % 4].astype(F32) + yz_r[u % SLOTS].astype(F32))
            near_copy(u).start()
            cross_copy(u).start()
            ze_copy(u).wait_send()

        u, when = stage(1 + 3 * LAG, end)

        @when
        def _(u=u):
            ze_copy(u).wait_recv()
            k = u % SLOTS
            yz_s[u % 4] = (z_own[k, span(z * zq, zq)] + ze_r[k].astype(F32)).astype(BF16)
            yz_copy(u).start()

        u, when = stage(1 + 2 * LAG, mid)

        @when
        def _(u=u):
            k = u % SLOTS
            zb_copy(u).wait_recv()
            zd_s[u % 4] = (y_own[k] + zb_r[k].astype(F32)).astype(BF16)
            zd_copy(u).start()
            zm_copy(u).wait()
            ze_s[u % 4] = (z_own[k, span(r_adj * zq, zq)] + zm_r[k, span((r_adj % 2) * zq, zq)].astype(F32)).astype(BF16)
            ze_copy(u).start()
            mine = span(z * zq, zq)
            yz_s[u % 4] = (z_own[k, mine] + za_r[k, mine].astype(F32) + zm_r[k, span((z % 2) * zq, zq)].astype(F32)).astype(BF16)
            yz_copy(u).start()

        u, when = stage(1 + 2 * LAG, end)

        @when
        def _(u=u):
            zb_copy(u).wait_send()

        u, when = stage(1 + LAG)

        @when
        def _(u=u):
            k = u % SLOTS
            y_copy(u).wait()

            @pl.when(end)
            def _():
                zb_s[u % 4] = (y_own[k] + y_r[k].astype(F32)).astype(BF16)
                zb_copy(u).start()
                za_copy(u).wait_send()

            @pl.when(mid)
            def _():
                za_copy(u).wait_recv()
                other = span((1 - side) * 2 * zq, 2 * zq)
                zm_s[u % 4] = (z_own[k, other] + za_r[k, other].astype(F32)).astype(BF16)
                zm_copy(u).start()
                y_own[k] = y_own[k] + y_r[k].astype(F32)

        @pl.when(t < units)
        def _():
            i = t // per_row

            @pl.when(jnp.logical_and(t % per_row == 0, t > 0))
            def _():
                a_copy(i).wait()

                @pl.when(i + 1 < mats * PARTS)
                def _():
                    a_copy(i + 1).start()

            @pl.when(t + 2 < units)
            def _():
                g_copy(t + 2).start()

            @pl.when(t == 0)
            def _():
                def chunk(i, _):
                    for copy in first_copies(i):
                        copy.wait()
                    some = span(i * tokens, tokens)
                    more = lax.dot_general(a_v[0, some], g_v[0, some], DN, preferred_element_type=F32)
                    part[0] = jnp.where(i == 0, more, part[0] + more)
                    return 0

                lax.fori_loop(0, CHUNKS, chunk, 0)

            @pl.when(t > 0)
            def _():
                g_copy(t).wait()
                part[t % 2] = lax.dot_general(a_v[i % 2], g_v[t % 3], DN, preferred_element_type=F32)

            d_s[t % 4] = part[t % 2, span((1 - c) * half, half), :].astype(BF16)
            d_copy(t).start()

        u, when = stage(1)

        @when
        def _(u=u):
            k = u % SLOTS
            p = u % 2
            d_copy(u).wait()
            there = (1 - y) * q
            here = y * q
            y_s[u % 4] = (part[p, span(c * half + there, q)] + d_r[k, span(there, q)].astype(F32)).astype(BF16)
            y_copy(u).start()

            @pl.when(end)
            def _():
                start = 2 * q + (1 - side) * zq
                za_s[u % 4] = (part[p, span(c * half + start, 3 * zq)] + d_r[k, span(start, 3 * zq)].astype(F32)).astype(BF16)
                za_copy(u).start()

            y_own[k] = part[p, span(c * half + here, q)] + d_r[k, span(here, q)].astype(F32)
            z_own[k] = part[p, span(c * half + 2 * q, 4 * zq)] + d_r[k, 2 * q:].astype(F32)

        return 0

    lax.fori_loop(0, units + 3 + 7 * LAG, step, 0)


def write(x, out, sems):
    mats, rows, _ = out.shape
    part = rows // WRITES
    copies = [pltpu.make_async_copy(x.at[n, pl.ds(i * part, part)], out.at[n, pl.ds(i * part, part)], sems.at[n, i])
              for n in range(mats) for i in range(WRITES)]
    for copy in copies:
        copy.start()
    for copy in copies:
        copy.wait()


def solution(mesh):
    def local(a, g):
        _, mats, tokens, depth = a.shape
        cols = g.shape[3]
        rows = depth // PARTS
        half = rows // 2
        zq = half // 10
        q = 3 * zq

        def buf(slots, n, dtype=BF16):
            return pltpu.VMEM((slots, n, W), dtype)

        def body(*refs):
            kernel(mats, q, zq, *refs)

        any_spec = pl.BlockSpec(memory_space=pl.ANY)
        dma = pltpu.SemaphoreType.DMA
        sums = pl.pallas_call(
            body,
            out_shape=pltpu.VMEM((mats, depth, cols), BF16),
            in_specs=[any_spec, any_spec],
            out_specs=pl.BlockSpec(memory_space=pltpu.VMEM),
            scratch_shapes=[
                pltpu.VMEM((2, tokens, rows), BF16),
                pltpu.VMEM((3, tokens, W), BF16),
                buf(2, rows, F32),
                buf(4, half), buf(SLOTS, half),
                buf(4, q), buf(SLOTS, q), buf(SLOTS, q, F32),
                buf(4, 3 * zq), buf(SLOTS, 4 * zq), buf(SLOTS, 4 * zq, F32),
                buf(4, q), buf(SLOTS, q),
                buf(4, 2 * zq), buf(SLOTS, 2 * zq),
                buf(4, q), buf(SLOTS, q),
                buf(4, zq), buf(SLOTS, zq),
                buf(4, zq), buf(SLOTS, zq),
                dma((2,)), dma((3,)), dma((2, CHUNKS)),
                dma((17, SEMS)), dma((17, SEMS)),
            ],
            compiler_params=pltpu.CompilerParams(collective_id=0, has_side_effects=True, vmem_limit_bytes=31 * 2**20),
            cost_estimate=pl.CostEstimate(flops=2 * mats * tokens * depth * cols, bytes_accessed=2 * mats * tokens * (depth + cols), transcendentals=0),
        )(a, g)
        return pl.pallas_call(
            write,
            out_shape=jax.ShapeDtypeStruct((mats, depth, cols), BF16),
            in_specs=[any_spec],
            out_specs=any_spec,
            scratch_shapes=[dma((mats, WRITES))],
            compiler_params=pltpu.CompilerParams(vmem_limit_bytes=2**20),
        )(sums)

    spec = P(("rep", "dp"))
    return jax.shard_map(local, mesh=mesh, in_specs=(spec, spec), out_specs=P("rep"), check_vma=False)
```

```python
import jax
import jax.numpy as jnp
from jax import lax
from jax.experimental import pallas as pl
from jax.experimental.pallas import tpu as pltpu
from jax.sharding import PartitionSpec as P

MESH = pl.DeviceIdType.MESH
BF16, F32 = jnp.bfloat16, jnp.float32
W = 256
PARTS = 2
SLOTS = 8
SEMS = 16
LATE = 2
CHUNKS = 4
LAG = 2
WRITES = 4
DN = (((0,), (0,)), ((), ()))


def kernel(mats, q, zq, a_hbm, g_hbm, out, a_v, g_v, part, d_s, d_r, y_s, y_r, y_own, za_s, za_r, z_own, zb_s, zb_r,
           zm_s, zm_r, zd_s, zd_r, ze_s, ze_r, yz_s, yz_r, a_sem, g_sem, first_sem, send_sem, recv_sem):
    rows = a_v.shape[2]
    half = rows // 2
    per_row = out.shape[2] // W
    units = mats * PARTS * per_row
    dp = lax.axis_index("dp")
    y, z, c = dp // 8, (dp // 2) % 4, dp % 2
    mid = jnp.logical_or(z == 1, z == 2)
    end = jnp.logical_not(mid)
    side = z // 2
    partner = dp + 1 - 2 * c
    yn = dp + 8 - 16 * y
    adj = dp + 2 - 4 * (z % 2)
    om = jnp.where(mid, dp + 6 - 4 * z, dp)
    r_adj = z + 1 - 2 * (z % 2)
    r_om = 3 - z
    r_far = r_om + 1 - 2 * (r_om % 2)

    far_mid = dp + 2 * (r_far - z)
    far_end = dp + 2 * (r_om - z)

    def span(start, n):
        return pl.ds(pl.multiple_of(start, 16), n)

    def rdma(kind, src, dst, u, to):
        return pltpu.make_async_remote_copy(
            src_ref=src, dst_ref=dst, send_sem=send_sem.at[kind, u % SEMS], recv_sem=recv_sem.at[kind, u % SEMS],
            device_id={"dp": to}, device_id_type=MESH)

    def place(u):
        n = u // (PARTS * per_row)
        return n, (u // per_row) % PARTS, pl.ds(pl.multiple_of((u % per_row) * W, W), W)

    def out_at(u, core, start, n):
        m, p, cols = place(u)
        return out.at[m, span(p * rows + core * half + start, n), cols]

    def final_copy(kind, core, start, n, to):
        def make(u):
            ref = out_at(u, core, start, n)
            return rdma(kind, ref, ref, u, to)

        return make

    def piece(r):
        return 2 * q + r * zq

    d_copy = lambda u: rdma(0, d_s.at[u % 4], d_r.at[u % SLOTS], u, partner)
    y_copy = lambda u: rdma(1, y_s.at[u % 4], y_r.at[u % SLOTS], u, yn)
    near_rows = span((1 - side) * zq, 3 * zq)
    za_copy = lambda u: rdma(2, za_s.at[u % 4], za_r.at[u % SLOTS, near_rows], u, adj)
    zb_copy = lambda u: rdma(3, zb_s.at[u % 4], zb_r.at[u % SLOTS], u, adj)
    zm_copy = lambda u: rdma(4, zm_s.at[u % 4], zm_r.at[u % SLOTS], u, om)
    zd_copy = lambda u: rdma(5, zd_s.at[u % 4], zd_r.at[u % SLOTS], u, om)
    ze_copy = lambda u: rdma(6, ze_s.at[u % 4], ze_r.at[u % SLOTS], u, adj)
    yz_copy = lambda u: rdma(7, yz_s.at[u % 4], yz_r.at[u % SLOTS], u, yn)
    z3_copy = final_copy(8, c, y * q, q, adj)
    ag_copy = final_copy(9, c, y * q, q, yn)
    ag_in = final_copy(9, c, (1 - y) * q, q, yn)
    near_copy = final_copy(10, c, piece(z), zq, adj)
    near_in = final_copy(10, c, piece(r_adj), zq, adj)
    cross_copy = final_copy(11, c, piece(z), zq, om)
    cross_in = final_copy(11, c, piece(r_om), zq, om)
    up_copy = final_copy(12, c, piece(z), zq, adj)
    up_in = final_copy(12, c, piece(r_adj), zq, adj)
    far1_copy = final_copy(13, c, piece(r_om), zq, adj)
    far1_in = final_copy(13, c, piece(r_far), zq, adj)
    over_copy = final_copy(14, c, piece(r_adj), zq, om)
    over_in = final_copy(14, c, piece(r_far), zq, om)
    far2_copy = final_copy(15, c, piece(r_far), zq, adj)
    far2_in = final_copy(15, c, piece(r_om), zq, adj)
    over_late = final_copy(14, c, piece(z), zq, far_mid)
    far2_late = final_copy(15, c, piece(z), zq, far_end)
    df_copy = final_copy(16, c, 0, half, partner)
    df_in = final_copy(16, 1 - c, 0, half, partner)

    def a_copy(i):
        src = a_hbm.at[0, i // PARTS, :, pl.ds(pl.multiple_of((i % PARTS) * rows, 128), rows)]
        return pltpu.make_async_copy(src, a_v.at[i % 2], a_sem.at[i % 2])

    def g_copy(u):
        m, _, cols = place(u)
        return pltpu.make_async_copy(g_hbm.at[0, m, :, cols], g_v.at[u % 3], g_sem.at[u % 3])

    def store(u, start, n, value):
        m, p, cols = place(u)
        out[m, span(p * rows + c * half + start, n), cols] = value.astype(BF16)

    tokens = a_v.shape[1] // CHUNKS

    def first_copies(i):
        some = span(i * tokens, tokens)
        return (pltpu.make_async_copy(a_hbm.at[0, 0, some, pl.ds(0, rows)], a_v.at[0, some], first_sem.at[0, i]),
                pltpu.make_async_copy(g_hbm.at[0, 0, some, pl.ds(0, W)], g_v.at[0, some], first_sem.at[1, i]))

    for i in range(CHUNKS):
        for copy in first_copies(i):
            copy.start()
    a_copy(1).start()
    g_copy(1).start()

    barrier = pltpu.get_barrier_semaphore()
    peers = [partner, yn] + [dp + 2 * ((z + i) % 4 - z) for i in range(1, 4)]
    for peer in peers:
        pl.semaphore_signal(barrier, inc=1, device_id={"dp": peer}, device_id_type=MESH)
    pl.semaphore_wait(barrier, len(peers))

    def step(t, _):
        def stage(off, who=None):
            u = t - off
            on = jnp.logical_and(u >= 0, u < units)
            return u, pl.when(on if who is None else jnp.logical_and(on, who))

        u, when = stage(3 + 7 * LAG)

        @when
        def _(u=u):
            df_copy(u).wait_send()
            df_in(u).wait_recv()

        u, when = stage(2 + 7 * LAG, mid)

        @when
        def _(u=u):
            @pl.when(u < units - LATE)
            def _():
                far2_copy(u).wait_send()

            df_copy(u).start()

        u, when = stage(2 + 7 * LAG, end)

        @when
        def _(u=u):
            far2_in(u).wait_recv()
            df_copy(u).start()

        u, when = stage(2 + 6 * LAG, mid)

        @when
        def _(u=u):
            over_in(u).wait_recv()

            @pl.when(u < units - LATE)
            def _():
                far2_copy(u).start()
                over_copy(u).wait_send()

        u, when = stage(2 + 5 * LAG)

        @when
        def _(u=u):
            @pl.when(mid)
            def _():
                up_in(u).wait_recv()

                @pl.when(u < units - LATE)
                def _():
                    over_copy(u).start()

                far1_copy(u).wait_send()

            @pl.when(end)
            def _():
                far1_in(u).wait_recv()
                up_copy(u).wait_send()

                @pl.when(u >= units - LATE)
                def _():
                    over_late(u).wait_send()
                    far2_late(u).wait_send()

            ag_copy(u).wait_send()
            ag_in(u).wait_recv()

        u, when = stage(2 + 4 * LAG, mid)

        @when
        def _(u=u):
            z3_copy(u).wait_send()
            ag_copy(u).start()
            cross_in(u).wait_recv()
            far1_copy(u).start()
            near_copy(u).wait_send()
            cross_copy(u).wait_send()

        u, when = stage(2 + 4 * LAG, end)

        @when
        def _(u=u):
            z3_copy(u).wait_recv()
            ag_copy(u).start()
            yz_copy(u).wait()
            store(u, piece(z), zq, yz_s[u % 4].astype(F32) + yz_r[u % SLOTS].astype(F32))
            up_copy(u).start()

            @pl.when(u >= units - LATE)
            def _():
                over_late(u).start()
                far2_late(u).start()

            near_in(u).wait_recv()

        u, when = stage(2 + 3 * LAG, mid)

        @when
        def _(u=u):
            zd_copy(u).wait()
            store(u, y * q, q, zd_s[u % 4].astype(F32) + zd_r[u % SLOTS].astype(F32))
            z3_copy(u).start()
            yz_copy(u).wait()
            store(u, piece(z), zq, yz_s[u % 4].astype(F32) + yz_r[u % SLOTS].astype(F32))
            near_copy(u).start()
            cross_copy(u).start()
            ze_copy(u).wait_send()

        u, when = stage(2 + 3 * LAG, end)

        @when
        def _(u=u):
            ze_copy(u).wait_recv()
            k = u % SLOTS
            yz_s[u % 4] = (z_own[k, span(z * zq, zq)] + ze_r[k].astype(F32)).astype(BF16)
            yz_copy(u).start()

        u, when = stage(2 + 2 * LAG, mid)

        @when
        def _(u=u):
            k = u % SLOTS
            zb_copy(u).wait_recv()
            zd_s[u % 4] = (y_own[k] + zb_r[k].astype(F32)).astype(BF16)
            zd_copy(u).start()
            zm_copy(u).wait()
            ze_s[u % 4] = (z_own[k, span(r_adj * zq, zq)] + zm_r[k, span((r_adj % 2) * zq, zq)].astype(F32)).astype(BF16)
            ze_copy(u).start()
            mine = span(z * zq, zq)
            yz_s[u % 4] = (z_own[k, mine] + za_r[k, mine].astype(F32) + zm_r[k, span((z % 2) * zq, zq)].astype(F32)).astype(BF16)
            yz_copy(u).start()

        u, when = stage(2 + 2 * LAG, end)

        @when
        def _(u=u):
            zb_copy(u).wait_send()

        u, when = stage(2 + LAG)

        @when
        def _(u=u):
            k = u % SLOTS
            y_copy(u).wait()

            @pl.when(end)
            def _():
                zb_s[u % 4] = (y_own[k] + y_r[k].astype(F32)).astype(BF16)
                zb_copy(u).start()
                za_copy(u).wait_send()

            @pl.when(mid)
            def _():
                za_copy(u).wait_recv()
                other = span((1 - side) * 2 * zq, 2 * zq)
                zm_s[u % 4] = (z_own[k, other] + za_r[k, other].astype(F32)).astype(BF16)
                zm_copy(u).start()
                y_own[k] = y_own[k] + y_r[k].astype(F32)

        @pl.when(t < units)
        def _():
            i = t // per_row

            @pl.when(jnp.logical_and(t % per_row == 0, t > 0))
            def _():
                a_copy(i).wait()

                @pl.when(i + 1 < mats * PARTS)
                def _():
                    a_copy(i + 1).start()

            @pl.when(t + 2 < units)
            def _():
                g_copy(t + 2).start()

            @pl.when(t == 0)
            def _():
                def chunk(i, _):
                    for copy in first_copies(i):
                        copy.wait()
                    some = span(i * tokens, tokens)
                    more = lax.dot_general(a_v[0, some], g_v[0, some], DN, preferred_element_type=F32)
                    part[0] = jnp.where(i == 0, more, part[0] + more)
                    return 0

                lax.fori_loop(0, CHUNKS, chunk, 0)

            @pl.when(t > 0)
            def _():
                g_copy(t).wait()
                part[t % 2] = lax.dot_general(a_v[i % 2], g_v[t % 3], DN, preferred_element_type=F32)

            d_s[t % 4] = part[t % 2, span((1 - c) * half, half), :].astype(BF16)
            d_copy(t).start()

        u, when = stage(1)

        @when
        def _(u=u):
            k = u % SLOTS
            p = u % 2
            d_copy(u).wait()
            there = (1 - y) * q
            here = y * q
            y_s[u % 4] = (part[p, span(c * half + there, q)] + d_r[k, span(there, q)].astype(F32)).astype(BF16)
            y_copy(u).start()

            @pl.when(end)
            def _():
                start = 2 * q + (1 - side) * zq
                za_s[u % 4] = (part[p, span(c * half + start, 3 * zq)] + d_r[k, span(start, 3 * zq)].astype(F32)).astype(BF16)
                za_copy(u).start()

            y_own[k] = part[p, span(c * half + here, q)] + d_r[k, span(here, q)].astype(F32)
            z_own[k] = part[p, span(c * half + 2 * q, 4 * zq)] + d_r[k, 2 * q:].astype(F32)

        return 0

    lax.fori_loop(0, units + 4 + 7 * LAG, step, 0)


def write(x, out, sems):
    mats, rows, _ = out.shape
    part = rows // WRITES
    copies = [pltpu.make_async_copy(x.at[n, pl.ds(i * part, part)], out.at[n, pl.ds(i * part, part)], sems.at[n, i])
              for n in range(mats) for i in range(WRITES)]
    for copy in copies:
        copy.start()
    for copy in copies:
        copy.wait()


def solution(mesh):
    def local(a, g):
        _, mats, tokens, depth = a.shape
        cols = g.shape[3]
        rows = depth // PARTS
        half = rows // 2
        zq = half // 10
        q = 3 * zq

        def buf(slots, n, dtype=BF16):
            return pltpu.VMEM((slots, n, W), dtype)

        def body(*refs):
            kernel(mats, q, zq, *refs)

        any_spec = pl.BlockSpec(memory_space=pl.ANY)
        dma = pltpu.SemaphoreType.DMA
        sums = pl.pallas_call(
            body,
            out_shape=pltpu.VMEM((mats, depth, cols), BF16),
            in_specs=[any_spec, any_spec],
            out_specs=pl.BlockSpec(memory_space=pltpu.VMEM),
            scratch_shapes=[
                pltpu.VMEM((2, tokens, rows), BF16),
                pltpu.VMEM((3, tokens, W), BF16),
                buf(2, rows, F32),
                buf(4, half), buf(SLOTS, half),
                buf(4, q), buf(SLOTS, q), buf(SLOTS, q, F32),
                buf(4, 3 * zq), buf(SLOTS, 4 * zq), buf(SLOTS, 4 * zq, F32),
                buf(4, q), buf(SLOTS, q),
                buf(4, 2 * zq), buf(SLOTS, 2 * zq),
                buf(4, q), buf(SLOTS, q),
                buf(4, zq), buf(SLOTS, zq),
                buf(4, zq), buf(SLOTS, zq),
                dma((2,)), dma((3,)), dma((2, CHUNKS)),
                dma((17, SEMS)), dma((17, SEMS)),
            ],
            compiler_params=pltpu.CompilerParams(collective_id=0, has_side_effects=True, vmem_limit_bytes=31 * 2**20),
            cost_estimate=pl.CostEstimate(flops=2 * mats * tokens * depth * cols, bytes_accessed=2 * mats * tokens * (depth + cols), transcendentals=0),
        )(a, g)
        return pl.pallas_call(
            write,
            out_shape=jax.ShapeDtypeStruct((mats, depth, cols), BF16),
            in_specs=[any_spec],
            out_specs=any_spec,
            scratch_shapes=[dma((mats, WRITES))],
            compiler_params=pltpu.CompilerParams(vmem_limit_bytes=2**20),
        )(sums)

    spec = P(("rep", "dp"))
    return jax.shard_map(local, mesh=mesh, in_specs=(spec, spec), out_specs=P("rep"), check_vma=False)
```
